32 devices in a mesh: dp: 8 (over z, y), mp: 4 (over x, core).
Axes of the slice: x: 2, y: 2, z: 4, core: 2. Of those that a mesh axis runs over, the one named last changes fastest.
Arguments:
- tokens: bfloat16 [8192, 4096], P('dp', 'mp'), may hold values from -6 to 6
- right_weight: bfloat16 [64, 64, 64], P('mp', 'dp'), may hold values from -0.75 to 0.75
- left_weight: bfloat16 [64, 64, 64], P('mp', 'dp'), may hold values from -0.75 to 0.75
- cotangent: bfloat16 [8192, 4096], P('dp', 'mp'), may hold values from -0.06591797 to 0.06591797
Outputs:
- activated: bfloat16 [8192, 4096], P('dp', 'mp')
- grad_right: float32 [64, 64, 64], P('mp', 'dp')
- grad_left: float32 [64, 64, 64], P('mp', 'dp')
The draws below stay inside these ranges and needn't reach their ends.
All inputs are finite; a program needn't handle non-finite values.
Results may differ from the reference program's by a relative error of at most 0.0056.
Values may be sent and summed in bfloat16 or wider, within the bound.
A program may use at most 64 MiB of HBM per device.

```python
import jax
import jax.numpy as jnp
from jax import lax

NB = 64
BS = 64
TOK_DEV = 1024
D = 4096
TOKENS = 8192
N_DP = 8


def block_scale(rng, dims, cuts, smallest, top_value):
    loudness, own = 1.0, jax.random.fold_in(rng, 6)
    for dim, shards_of in cuts:
        heights = jnp.exp(jax.random.uniform(jax.random.fold_in(own, dim), (shards_of,), jnp.float32, smallest / len(cuts), top_value / len(cuts)))
        loudness = loudness * jnp.repeat(heights, dims[dim] // shards_of).reshape([-1 if axis == dim else 1 for axis in range(len(dims))])
    return loudness


def scatter_about(rng, dims, width, limit, shards=(), dtype=jnp.bfloat16):
    result = width * jax.random.normal(rng, dims, jnp.float32)
    if shards:
        result = result * block_scale(rng, dims, shards, -0.22, 0.18)
    return jnp.clip(result, -limit, limit).astype(dtype)


def setup_inputs(seed: int = 0) -> dict:
    keys = jax.random.split(jax.random.key(seed), 5)
    return {
        "tokens": scatter_about(keys[0], (TOKENS, D), 1.0, 6.0, ((0, 8), (1, 4))),
        "right_weight": scatter_about(keys[1], (NB, BS, BS), BS ** -0.5, 0.75, ((0, 4), (1, 8))),
        "left_weight": scatter_about(keys[2], (BS, NB, BS), NB ** -0.5, 0.75, ((0, 4), (1, 8))),
        "cotangent": scatter_about(keys[3], (TOKENS, D), ((TOK_DEV * N_DP) ** -0.5), 0.06591797, ((0, 8), (1, 4))),
    }


def gelu_slope(pre):
    cdf = 0.5 * (1.0 + lax.erf(pre * 0.7071067811865476))
    density = jnp.exp(-0.5 * pre * pre) * 0.3989422804014327
    return cdf + pre * density


def reference(tokens, right_weight, left_weight, cotangent):
    right_f = right_weight.astype(jnp.float32)
    left_f = left_weight.astype(jnp.float32)
    xs_all = tokens.reshape(N_DP, TOK_DEV, NB, BS)
    gs_all = cotangent.reshape(N_DP, TOK_DEV, BS, BS)

    def step(carry, pieces):
        grad_r, grad_l = carry
        xs, gs = pieces
        xs_f = xs.astype(jnp.float32)
        inner = jnp.einsum('tik,ikm->tim', xs_f, right_f).astype(jnp.bfloat16)
        inner_f = inner.astype(jnp.float32)
        pre = jnp.einsum('tim,min->tmn', inner_f, left_f)
        activated = jax.nn.gelu(pre, approximate=False).astype(jnp.bfloat16)
        dpre = (gs.astype(jnp.float32) * gelu_slope(pre)).astype(jnp.bfloat16)
        dpre_f = dpre.astype(jnp.float32)
        grad_l = grad_l + jnp.einsum('tim,tmn->min', inner_f, dpre_f)
        dinner = jnp.einsum('tmn,min->tim', dpre_f, left_f).astype(jnp.bfloat16)
        grad_r = grad_r + jnp.einsum('tik,tim->ikm', xs_f, dinner.astype(jnp.float32))
        return (grad_r, grad_l), activated

    start = (jnp.zeros((NB, BS, BS), jnp.float32), jnp.zeros((BS, NB, BS), jnp.float32))
    (grad_right, grad_left), outs = lax.scan(step, start, (xs_all, gs_all))
    activated = outs.reshape(N_DP * TOK_DEV, NB * BS)
    return activated, grad_right, grad_left
```

```python
import functools

import jax
import jax.numpy as jnp
from jax import lax
from jax.experimental import pallas as pl
from jax.experimental.pallas import tpu as pltpu
from jax.sharding import PartitionSpec as P

MESH = pl.DeviceIdType.MESH
BF = jnp.bfloat16
F32 = jnp.float32
CHUNKS = 8


def iota(shape, dim):
    return lax.broadcasted_iota(jnp.int32, shape, dim)


def ones_where(cond):
    return jnp.where(cond, 1.0, 0.0).astype(BF)


def dot_nn(a, b):
    return lax.dot_general(a, b, (((1,), (0,)), ((), ())), preferred_element_type=F32)


def dot_nt(a, b):
    return lax.dot_general(a, b, (((1,), (1,)), ((), ())), preferred_element_type=F32)


def dot_tn(a, b):
    return lax.dot_general(a, b, (((0,), (0,)), ((), ())), preferred_element_type=F32)


def join(parts, axis=1):
    return parts[0] if len(parts) == 1 else jnp.concatenate(parts, axis=axis)


class Sizes:
    def __init__(self, n_dp, n_mp, tok_rows, features, width):
        self.dp, self.mp = n_dp, n_mp
        self.tok, self.feat, self.bs = tok_rows, features, width
        self.own = features // width
        self.blocks = self.own * n_mp
        self.rows = width // n_dp
        self.orow = self.own * self.rows
        self.pad = max(self.own, 16)
        self.gs = max(1, 128 // (self.own * self.own))
        self.groups = n_mp // self.gs
        self.ng = self.gs * self.own * self.own
        self.kg = self.gs * features
        self.jg = self.ng // 128
        self.jl = self.own // self.jg
        self.nj = self.ng // self.jg
        self.rh = self.groups * self.nj
        self.fj = self.jl * width
        self.n = n_dp * n_mp
        self.tc = tok_rows // CHUNKS


def kernel(z, x_hbm, cot_hbm, rw_hbm, lw_hbm, act_hbm, gr_ref, gl_ref,
           xfull, cot, act, rg, lg, p1, p2, wt, lt, gracc, glacc,
           rsend, rrecv, lsend, lrecv,
           x_recv, x_send, x_local, c_local, a_out,
           rw_send, rw_recv, lw_send, lw_recv, gr_send, gr_recv, gl_send, gl_recv):
    d, p = lax.axis_index("dp"), lax.axis_index("mp")
    me = d * z.mp + p
    core = lax.rem(p, 2)
    partner = p + 1 - 2 * core
    chip = p // 2
    chips = z.mp // 2

    barrier = pltpu.get_barrier_semaphore()

    @pl.loop(1, z.n)
    def _(s):
        o = lax.rem(me + s, z.n)
        pl.semaphore_signal(barrier, inc=1, device_id=(o // z.mp, lax.rem(o, z.mp)), device_id_type=MESH)

    def rows(c):
        return pl.ds(pl.multiple_of(c * z.tc, z.tc), z.tc)

    def local_x(c):
        return pltpu.make_async_copy(x_hbm.at[rows(c)], xfull.at[p, rows(c)], x_local.at[c])

    def local_c(c):
        return pltpu.make_async_copy(cot_hbm.at[rows(c)], cot.at[rows(c)], c_local.at[c])

    def out_act(c):
        return pltpu.make_async_copy(act.at[rows(c)], act_hbm.at[rows(c)], a_out.at[c])

    def send_own(c, kind, target):
        return pltpu.make_async_remote_copy(
            src_ref=x_hbm.at[rows(c)], dst_ref=xfull.at[p, rows(c)],
            send_sem=x_send.at[kind, c], recv_sem=x_recv.at[p, c],
            device_id=(d, target), device_id_type=MESH)

    def forward(c, kind, source):
        return pltpu.make_async_remote_copy(
            src_ref=xfull.at[source, rows(c)], dst_ref=xfull.at[source, rows(c)],
            send_sem=x_send.at[kind, c], recv_sem=x_recv.at[source, c],
            device_id=(d, partner), device_id_type=MESH)

    def arrived(c, source):
        pltpu.make_async_remote_copy(
            src_ref=xfull.at[source, rows(c)], dst_ref=xfull.at[source, rows(c)],
            send_sem=x_send.at[0, c], recv_sem=x_recv.at[source, c],
            device_id=(d, partner), device_id_type=MESH).wait_recv()

    def same_core(s):
        return lax.rem(chip + s, chips) * 2 + core

    def other_core(s):
        return lax.rem(chip + s, chips) * 2 + 1 - core

    @pl.loop(0, CHUNKS)
    def _(c):
        local_x(c).start()
        local_c(c).start()

    pl.semaphore_wait(barrier, z.n - 1)

    own_rw = pltpu.make_async_copy(rw_hbm.at[p], rg.at[me], rw_recv)
    own_rw.start()
    own_lw = pltpu.make_async_copy(lw_hbm, lg.at[d], lw_recv)
    own_lw.start()

    @pl.loop(1, z.n)
    def _(s):
        o = lax.rem(me + s, z.n)
        q = lax.rem(o, z.mp)
        pltpu.make_async_remote_copy(
            src_ref=rw_hbm.at[q], dst_ref=rg.at[me], send_sem=rw_send, recv_sem=rw_recv,
            device_id=(o // z.mp, q), device_id_type=MESH).start()

    @pl.loop(1, z.dp)
    def _(s):
        pltpu.make_async_remote_copy(
            src_ref=lw_hbm, dst_ref=lg.at[d], send_sem=lw_send, recv_sem=lw_recv,
            device_id=(lax.rem(d + s, z.dp), p), device_id_type=MESH).start()

    @pl.loop(0, CHUNKS)
    def _(c):
        for s in range(1, chips):
            send_own(c, s, same_core(s)).start()
        send_own(c, 0, partner).start()

    for dd in range(z.dp):
        shape = (z.orow, z.feat)
        a, b = iota(shape, 0), iota(shape, 1)
        source = (b // z.bs) * z.rows + (b % z.bs) - dd * z.rows
        inside = (b % z.bs) // z.rows == dd
        p1[dd] = ones_where(inside & (a == source))
        shape = (z.orow, z.blocks * z.own)
        a, b = iota(shape, 0), iota(shape, 1)
        jg = b // z.rh
        i_all = (b % z.rh) // z.jl
        j = jg * z.jl + b % z.jl
        inside = i_all // z.rows == dd
        p2[dd] = ones_where(inside & (a == j * z.rows + i_all % z.rows))
    gracc[...] = jnp.zeros_like(gracc)
    glacc[...] = jnp.zeros_like(glacc)

    def count(ref, sem):
        pltpu.make_async_copy(ref, ref, sem).wait()

    count(lg, lw_recv)
    left = None
    for dd in range(z.dp):
        part = dot_nn(lg[dd], p2[dd])
        left = part if left is None else left + part
    left = left.astype(BF)
    shape = (z.fj, z.bs)
    spread = ones_where(iota(shape, 0) % z.bs == iota(shape, 1))
    for jg in range(z.jg):
        piece = dot_nn(spread, left[:, jg * z.rh:(jg + 1) * z.rh])
        keep = iota((z.fj, z.rh), 0) // z.bs == iota((z.fj, z.rh), 1) % z.jl
        lt[jg] = jnp.where(keep, piece, 0.0).astype(BF)

    count(rg, rw_recv)
    right = None
    for dd in range(z.dp):
        part = dot_nn(rg[dd * z.mp:(dd + 1) * z.mp].reshape(z.mp * z.pad, z.orow), p1[dd])
        right = part if right is None else right + part
    right = right.astype(BF)
    for g in range(z.groups):
        for s in range(z.gs):
            shape = (z.ng, z.mp * z.pad)
            a, b = iota(shape, 0), iota(shape, 1)
            j = (a // z.nj) * z.jl + a % z.jl
            src = (a % z.nj) // (z.own * z.jl)
            pick = ones_where((src == s) & (b == (g * z.gs + s) * z.pad + j))
            piece = dot_nn(pick, right)
            shape = (z.ng, z.feat)
            keep = (iota(shape, 0) // z.jl) % z.own == iota(shape, 1) // z.bs
            wt[g, :, s * z.feat:(s + 1) * z.feat] = jnp.where(keep, piece, 0.0).astype(BF)

    @pl.loop(0, CHUNKS)
    def _(c):
        local_x(c).wait()
        local_c(c).wait()
        for s in range(1, chips):
            arrived(c, same_core(s))
            forward(c, chips + s, same_core(s)).start()
        arrived(c, partner)
        for s in range(1, chips):
            arrived(c, other_core(s))
        r = rows(c)
        xs = [join([xfull[g * z.gs + s, r] for s in range(z.gs)]) for g in range(z.groups)]
        inner = [dot_nt(xs[g], wt[g]).astype(BF) for g in range(z.groups)]
        back = []
        for jg in range(z.jg):
            mixed = join([v[:, jg * z.nj:(jg + 1) * z.nj] for v in inner])
            pre = dot_nt(mixed, lt[jg])
            cdf = 0.5 * (1.0 + lax.erf(pre * 0.7071067811865476))
            slope = cdf + pre * (jnp.exp(-0.5 * pre * pre) * 0.3989422804014327)
            cols = pl.ds(jg * z.fj, z.fj)
            act[r, cols] = (pre * cdf).astype(BF)
            dpre = (cot[r, cols].astype(F32) * slope).astype(BF)
            glacc[jg] += dot_tn(dpre, mixed)
            back.append(dot_nn(dpre, lt[jg]).astype(BF))
        out_act(c).start()
        for g in range(z.groups):
            dinner = join([v[:, g * z.nj:(g + 1) * z.nj] for v in back])
            gracc[g] += dot_tn(dinner, xs[g])

    shape = (z.bs, z.fj)
    fold = ones_where(iota(shape, 1) % z.bs == iota(shape, 0))
    lefts = []
    for jg in range(z.jg):
        keep = iota((z.fj, z.rh), 0) // z.bs == iota((z.fj, z.rh), 1) % z.jl
        lefts.append(dot_nn(fold, jnp.where(keep, glacc[jg], 0.0).astype(BF)).astype(BF))
    left = join(lefts)
    for dd in range(z.dp):
        lsend[dd] = dot_nt(left, p2[dd]).astype(BF)

    @pl.loop(1, z.dp)
    def _(s):
        o = lax.rem(d + s, z.dp)
        pltpu.make_async_remote_copy(
            src_ref=lsend.at[o], dst_ref=lrecv.at[d], send_sem=gl_send, recv_sem=gl_recv,
            device_id=(o, p), device_id_type=MESH).start()

    for g in range(z.groups):
        for s in range(z.gs):
            shape = (z.pad, z.ng)
            a, b = iota(shape, 0), iota(shape, 1)
            j = (b // z.nj) * z.jl + b % z.jl
            src = (b % z.nj) // (z.own * z.jl)
            pick = ones_where((src == s) & (a == j))
            shape = (z.ng, z.feat)
            keep = (iota(shape, 0) // z.jl) % z.own == iota(shape, 1) // z.bs
            piece = jnp.where(keep, gracc[g, :, s * z.feat:(s + 1) * z.feat], 0.0).astype(BF)
            piece = dot_nn(pick, piece).astype(BF)
            for dd in range(z.dp):
                rsend[dd * z.mp + g * z.gs + s] = dot_nt(piece, p1[dd]).astype(BF)

    @pl.loop(1, z.n)
    def _(s):
        o = lax.rem(me + s, z.n)
        pltpu.make_async_remote_copy(
            src_ref=rsend.at[o], dst_ref=rrecv.at[me], send_sem=gr_send, recv_sem=gr_recv,
            device_id=(o // z.mp, lax.rem(o, z.mp)), device_id_type=MESH).start()

    lrecv[d] = lsend[d]
    rrecv[me] = rsend[me]

    @pl.loop(0, CHUNKS)
    def _(c):
        for s in range(1, chips):
            send_own(c, s, same_core(s)).wait_send()
            forward(c, chips + s, same_core(s)).wait_send()
        send_own(c, 0, partner).wait_send()
        out_act(c).wait()

    count(rg.at[pl.ds(0, z.n - 1)], rw_send)
    count(lg.at[pl.ds(0, z.dp - 1)], lw_send)

    count(lrecv.at[pl.ds(0, z.dp - 1)], gl_recv)
    total = lrecv[0].astype(F32)
    for dd in range(1, z.dp):
        total = total + lrecv[dd].astype(F32)
    gl_ref[...] = total
    count(rrecv.at[pl.ds(0, z.n - 1)], gr_recv)
    total = rrecv[0:z.mp].astype(F32)
    for dd in range(1, z.dp):
        total = total + rrecv[dd * z.mp:(dd + 1) * z.mp].astype(F32)
    gr_ref[...] = total
    count(lsend.at[pl.ds(0, z.dp - 1)], gl_send)
    count(rsend.at[pl.ds(0, z.n - 1)], gr_send)


def shards(z, tokens, right_weight, left_weight, cotangent):
    rw = right_weight.transpose(2, 0, 1).reshape(z.mp, z.own, z.orow)
    rw = jnp.pad(rw, ((0, 0), (0, z.pad - z.own), (0, 0)))
    lw = left_weight.transpose(2, 0, 1).reshape(z.bs, z.orow)
    hbm = pl.BlockSpec(memory_space=pltpu.HBM)
    vmem = pl.BlockSpec(memory_space=pltpu.VMEM)
    dma = pltpu.SemaphoreType.DMA
    act, gr, gl = pl.pallas_call(
        functools.partial(kernel, z),
        out_shape=(
            jax.ShapeDtypeStruct((z.tok, z.feat), BF),
            jax.ShapeDtypeStruct((z.mp, z.pad, z.orow), F32),
            jax.ShapeDtypeStruct((z.bs, z.orow), F32),
        ),
        in_specs=[hbm] * 4,
        out_specs=(hbm, vmem, vmem),
        scratch_shapes=[
            pltpu.VMEM((z.mp, z.tok, z.feat), BF),
            pltpu.VMEM((z.tok, z.feat), BF),
            pltpu.VMEM((z.tok, z.feat), BF),
            pltpu.VMEM((z.n, z.pad, z.orow), BF),
            pltpu.VMEM((z.dp, z.bs, z.orow), BF),
            pltpu.VMEM((z.dp, z.orow, z.feat), BF),
            pltpu.VMEM((z.dp, z.orow, z.blocks * z.own), BF),
            pltpu.VMEM((z.groups, z.ng, z.kg), BF),
            pltpu.VMEM((z.jg, z.fj, z.rh), BF),
            pltpu.VMEM((z.groups, z.ng, z.kg), F32),
            pltpu.VMEM((z.jg, z.fj, z.rh), F32),
            pltpu.VMEM((z.n, z.pad, z.orow), BF),
            pltpu.VMEM((z.n, z.pad, z.orow), BF),
            pltpu.VMEM((z.dp, z.bs, z.orow), BF),
            pltpu.VMEM((z.dp, z.bs, z.orow), BF),
            dma((z.mp, CHUNKS)),
            dma((z.mp, CHUNKS)),
            dma((CHUNKS,)),
            dma((CHUNKS,)),
            dma((CHUNKS,)),
            dma, dma, dma, dma, dma, dma, dma, dma,
        ],
        compiler_params=pltpu.CompilerParams(
            collective_id=0, has_side_effects=True, vmem_limit_bytes=60 * 1024 * 1024),
    )(tokens, cotangent, rw, lw)
    gr = gr[:, :z.own].reshape(z.mp * z.own, z.own, z.rows).transpose(1, 2, 0)
    gl = gl.reshape(z.bs, z.own, z.rows).transpose(1, 2, 0)
    return act, gr, gl


def solution(mesh):
    n_dp, n_mp = mesh.shape["dp"], mesh.shape["mp"]

    def step(tokens, right_weight, left_weight, cotangent):
        z = Sizes(n_dp, n_mp, tokens.shape[0] // n_dp, tokens.shape[1] // n_mp, right_weight.shape[1])
        return jax.shard_map(
            functools.partial(shards, z),
            mesh=mesh,
            in_specs=(P("dp", "mp"), P("mp", "dp", None), P("mp", "dp", None), P("dp", "mp")),
            out_specs=(P("dp", "mp"), P("mp", "dp", None), P("mp", "dp", None)),
            check_vma=False,
        )(tokens, right_weight, left_weight, cotangent)

    return step
```

```python
import functools

import jax
import jax.numpy as jnp
from jax import lax
from jax.experimental import pallas as pl
from jax.experimental.pallas import tpu as pltpu
from jax.sharding import PartitionSpec as P

MESH = pl.DeviceIdType.MESH
BF = jnp.bfloat16
F32 = jnp.float32
CHUNKS = 8


def iota(shape, dim):
    line = tuple(n if axis == dim else 1 for axis, n in enumerate(shape))
    return lax.broadcasted_iota(jnp.int32, line, dim)


def ones_where(cond):
    return jnp.where(cond, 1.0, 0.0).astype(BF)


def dot_nn(a, b):
    return lax.dot_general(a, b, (((1,), (0,)), ((), ())), preferred_element_type=F32)


def dot_nt(a, b):
    return lax.dot_general(a, b, (((1,), (1,)), ((), ())), preferred_element_type=F32)


def dot_tn(a, b):
    return lax.dot_general(a, b, (((0,), (0,)), ((), ())), preferred_element_type=F32)


def join(parts, axis=1):
    return parts[0] if len(parts) == 1 else jnp.concatenate(parts, axis=axis)


class Sizes:
    def __init__(self, n_dp, n_mp, tok_rows, features, width):
        self.dp, self.mp = n_dp, n_mp
        self.tok, self.feat, self.bs = tok_rows, features, width
        self.own = features // width
        self.blocks = self.own * n_mp
        self.rows = width // n_dp
        self.orow = self.own * self.rows
        self.pad = max(self.own, 16)
        self.gs = max(1, 128 // (self.own * self.own))
        self.groups = n_mp // self.gs
        self.ng = self.gs * self.own * self.own
        self.kg = self.gs * features
        self.jg = self.ng // 128
        self.jl = self.own // self.jg
        self.nj = self.ng // self.jg
        self.rh = self.groups * self.nj
        self.fj = self.jl * width
        self.n = n_dp * n_mp
        self.direct = self.pad == self.own and self.orow % 128 == 0
        self.tc = tok_rows // CHUNKS


def kernel(z, x_hbm, cot_hbm, rw_hbm, lw_hbm, act_hbm, gr_ref, gl_ref,
           xfull, cot, act, rw_v, lw_v, rwt, lwt, rg, lg, p1, p2, wt, lt, gracc, glacc,
           rsend, rrecv, lsend, lrecv,
           x_recv, x_send, x_local, c_local, a_out, w_local,
           rw_send, rw_recv, lw_send, lw_recv, gr_send, gr_recv, gl_send, gl_recv):
    d, p = lax.axis_index("dp"), lax.axis_index("mp")
    me = d * z.mp + p
    core = lax.rem(p, 2)
    partner = p + 1 - 2 * core
    chip = p // 2
    chips = z.mp // 2

    barrier = pltpu.get_barrier_semaphore()

    @pl.loop(1, z.n)
    def _(s):
        o = lax.rem(me + s, z.n)
        pl.semaphore_signal(barrier, inc=1, device_id=(o // z.mp, lax.rem(o, z.mp)), device_id_type=MESH)

    def rows(c):
        return pl.ds(pl.multiple_of(c * z.tc, z.tc), z.tc)

    def local_x(c):
        return pltpu.make_async_copy(x_hbm.at[rows(c)], xfull.at[p, rows(c)], x_local.at[c])

    def local_c(c):
        return pltpu.make_async_copy(cot_hbm.at[rows(c)], cot.at[rows(c)], c_local.at[c])

    def out_act(c):
        return pltpu.make_async_copy(act.at[rows(c)], act_hbm.at[rows(c)], a_out.at[c])

    def send_own(c, kind, target):
        return pltpu.make_async_remote_copy(
            src_ref=x_hbm.at[rows(c)], dst_ref=xfull.at[p, rows(c)],
            send_sem=x_send.at[kind, c], recv_sem=x_recv.at[p, c],
            device_id=(d, target), device_id_type=MESH)

    def forward(c, kind, source):
        return pltpu.make_async_remote_copy(
            src_ref=xfull.at[source, rows(c)], dst_ref=xfull.at[source, rows(c)],
            send_sem=x_send.at[kind, c], recv_sem=x_recv.at[source, c],
            device_id=(d, partner), device_id_type=MESH)

    def arrived(c, source):
        pltpu.make_async_remote_copy(
            src_ref=xfull.at[source, rows(c)], dst_ref=xfull.at[source, rows(c)],
            send_sem=x_send.at[0, c], recv_sem=x_recv.at[source, c],
            device_id=(d, partner), device_id_type=MESH).wait_recv()

    def same_core(s):
        return lax.rem(chip + s, chips) * 2 + core

    def other_core(s):
        return lax.rem(chip + s, chips) * 2 + 1 - core

    @pl.loop(0, CHUNKS)
    def _(c):
        local_x(c).start()
        local_c(c).start()

    local_r = pltpu.make_async_copy(rw_hbm, rw_v, w_local.at[0])
    local_r.start()
    local_l = pltpu.make_async_copy(lw_hbm, lw_v, w_local.at[1])
    local_l.start()
    local_r.wait()
    local_l.wait()
    shape = (z.mp * z.pad, z.bs)
    a, b = iota(shape, 0), iota(shape, 1)
    wide = ones_where((a % z.pad < z.own) & (b == (a // z.pad) * z.own + a % z.pad))
    rwt[...] = dot_nt(wide, rw_v[...]).astype(BF).reshape(z.mp, z.pad, z.orow)
    shape = (z.bs, z.bs)
    lwt[...] = dot_nt(ones_where(iota(shape, 0) == iota(shape, 1)), lw_v[...]).astype(BF)
    rg[me] = rwt[p]
    lg[d] = lwt[...]

    pl.semaphore_wait(barrier, z.n - 1)

    def send_x(c):
        for s in range(1, chips):
            send_own(c, s, same_core(s)).start()
        send_own(c, 0, partner).start()

    send_x(0)

    @pl.loop(1, z.n)
    def _(s):
        o = lax.rem(me + s, z.n)
        q = lax.rem(o, z.mp)
        pltpu.make_async_remote_copy(
            src_ref=rwt.at[q], dst_ref=rg.at[me], send_sem=rw_send, recv_sem=rw_recv,
            device_id=(o // z.mp, q), device_id_type=MESH).start()

    @pl.loop(1, z.dp)
    def _(s):
        pltpu.make_async_remote_copy(
            src_ref=lwt, dst_ref=lg.at[d], send_sem=lw_send, recv_sem=lw_recv,
            device_id=(lax.rem(d + s, z.dp), p), device_id_type=MESH).start()

    @pl.loop(1, CHUNKS)
    def _(c):
        send_x(c)

    for dd in range(z.dp):
        shape = (z.orow, z.feat)
        a, b = iota(shape, 0), iota(shape, 1)
        source = (b // z.bs) * z.rows + (b % z.bs) - dd * z.rows
        inside = (b % z.bs) // z.rows == dd
        p1[dd] = ones_where(inside & (a == source))
        shape = (z.orow, z.blocks * z.own)
        a, b = iota(shape, 0), iota(shape, 1)
        jg = b // z.rh
        i_all = (b % z.rh) // z.jl
        j = jg * z.jl + b % z.jl
        inside = i_all // z.rows == dd
        p2[dd] = ones_where(inside & (a == j * z.rows + i_all % z.rows))
    gracc[...] = jnp.zeros_like(gracc)
    glacc[...] = jnp.zeros_like(glacc)

    def count(ref, sem):
        pltpu.make_async_copy(ref, ref, sem).wait()

    count(lg.at[pl.ds(0, z.dp - 1)], lw_recv)
    left = None
    for dd in range(z.dp):
        part = dot_nn(lg[dd], p2[dd])
        left = part if left is None else left + part
    left = left.astype(BF)
    shape = (z.fj, z.bs)
    spread = ones_where(iota(shape, 0) % z.bs == iota(shape, 1))
    for jg in range(z.jg):
        piece = dot_nn(spread, left[:, jg * z.rh:(jg + 1) * z.rh])
        keep = iota((z.fj, z.rh), 0) // z.bs == iota((z.fj, z.rh), 1) % z.jl
        lt[jg] = jnp.where(keep, piece, 0.0).astype(BF)

    count(rg.at[pl.ds(0, z.n - 1)], rw_recv)
    right = None
    for dd in range(z.dp):
        part = dot_nn(rg[dd * z.mp:(dd + 1) * z.mp].reshape(z.mp * z.pad, z.orow), p1[dd])
        right = part if right is None else right + part
    right = right.astype(BF)
    for g in range(z.groups):
        for s in range(z.gs):
            shape = (z.ng, z.mp * z.pad)
            a, b = iota(shape, 0), iota(shape, 1)
            j = (a // z.nj) * z.jl + a % z.jl
            src = (a % z.nj) // (z.own * z.jl)
            pick = ones_where((src == s) & (b == (g * z.gs + s) * z.pad + j))
            piece = dot_nn(pick, right)
            shape = (z.ng, z.feat)
            keep = (iota(shape, 0) // z.jl) % z.own == iota(shape, 1) // z.bs
            wt[g, :, s * z.feat:(s + 1) * z.feat] = jnp.where(keep, piece, 0.0).astype(BF)

    @pl.loop(0, CHUNKS)
    def _(c):
        local_x(c).wait()
        local_c(c).wait()
        for s in range(1, chips):
            arrived(c, same_core(s))
            forward(c, chips + s, same_core(s)).start()
        arrived(c, partner)
        for s in range(1, chips):
            arrived(c, other_core(s))
        r = rows(c)
        xs = [join([xfull[g * z.gs + s, r] for s in range(z.gs)]) for g in range(z.groups)]
        inner = [dot_nt(xs[g], wt[g]).astype(BF) for g in range(z.groups)]
        back = []
        for jg in range(z.jg):
            mixed = join([v[:, jg * z.nj:(jg + 1) * z.nj] for v in inner])
            pre = dot_nt(mixed, lt[jg])
            cdf = 0.5 * (1.0 + lax.erf(pre * 0.7071067811865476))
            slope = cdf + pre * (jnp.exp(-0.5 * pre * pre) * 0.3989422804014327)
            cols = pl.ds(jg * z.fj, z.fj)
            act[r, cols] = (pre * cdf).astype(BF)
            dpre = (cot[r, cols].astype(F32) * slope).astype(BF)
            glacc[jg] += dot_tn(dpre, mixed)
            back.append(dot_nn(dpre, lt[jg]).astype(BF))
        out_act(c).start()
        for g in range(z.groups):
            dinner = join([v[:, g * z.nj:(g + 1) * z.nj] for v in back])
            gracc[g] += dot_tn(dinner, xs[g])

    shape = (z.bs, z.fj)
    fold = ones_where(iota(shape, 1) % z.bs == iota(shape, 0))
    lefts = []
    for jg in range(z.jg):
        keep = iota((z.fj, z.rh), 0) // z.bs == iota((z.fj, z.rh), 1) % z.jl
        lefts.append(dot_nn(fold, jnp.where(keep, glacc[jg], 0.0).astype(BF)).astype(BF))
    left = join(lefts)
    for dd in range(z.dp):
        lsend[dd] = dot_nt(left, p2[dd]).astype(BF)

    @pl.loop(1, z.dp)
    def _(s):
        o = lax.rem(d + s, z.dp)
        pltpu.make_async_remote_copy(
            src_ref=lsend.at[o], dst_ref=lrecv.at[d], send_sem=gl_send, recv_sem=gl_recv,
            device_id=(o, p), device_id_type=MESH).start()

    pieces = []
    for g in range(z.groups):
        for s in range(z.gs):
            shape = (z.pad, z.ng)
            a, b = iota(shape, 0), iota(shape, 1)
            j = (b // z.nj) * z.jl + b % z.jl
            src = (b % z.nj) // (z.own * z.jl)
            pick = ones_where((src == s) & (a == j))
            shape = (z.ng, z.feat)
            keep = (iota(shape, 0) // z.jl) % z.own == iota(shape, 1) // z.bs
            piece = jnp.where(keep, gracc[g, :, s * z.feat:(s + 1) * z.feat], 0.0).astype(BF)
            pieces.append(dot_nn(pick, piece).astype(BF))
    pieces = join(pieces, axis=0)
    for dd in range(z.dp):
        owned = dot_nt(pieces, p1[dd]).astype(BF)
        rsend[dd * z.mp:(dd + 1) * z.mp] = owned.reshape(z.mp, z.pad, z.orow)

    @pl.loop(1, z.n)
    def _(s):
        o = lax.rem(me + s, z.n)
        pltpu.make_async_remote_copy(
            src_ref=rsend.at[o], dst_ref=rrecv.at[me], send_sem=gr_send, recv_sem=gr_recv,
            device_id=(o // z.mp, lax.rem(o, z.mp)), device_id_type=MESH).start()

    lrecv[d] = lsend[d]
    rrecv[me] = rsend[me]

    @pl.loop(0, CHUNKS)
    def _(c):
        for s in range(1, chips):
            send_own(c, s, same_core(s)).wait_send()
            forward(c, chips + s, same_core(s)).wait_send()
        send_own(c, 0, partner).wait_send()
        out_act(c).wait()

    count(rg.at[pl.ds(0, z.n - 1)], rw_send)
    count(lg.at[pl.ds(0, z.dp - 1)], lw_send)

    count(lrecv.at[pl.ds(0, z.dp - 1)], gl_recv)
    total = lrecv[0].astype(F32)
    for dd in range(1, z.dp):
        total = total + lrecv[dd].astype(F32)
    gl_ref[...] = total.T if z.direct else total
    count(rrecv.at[pl.ds(0, z.n - 1)], gr_recv)
    total = rrecv[0:z.mp].astype(F32)
    for dd in range(1, z.dp):
        total = total + rrecv[dd * z.mp:(dd + 1) * z.mp].astype(F32)
    gr_ref[...] = total.reshape(z.blocks, z.orow).T if z.direct else total
    count(lsend.at[pl.ds(0, z.dp - 1)], gl_send)
    count(rsend.at[pl.ds(0, z.n - 1)], gr_send)


def shards(z, tokens, right_weight, left_weight, cotangent):
    rw = right_weight.reshape(z.orow, z.bs)
    lw = left_weight.reshape(z.orow, z.bs)
    hbm = pl.BlockSpec(memory_space=pltpu.HBM)
    vmem = pl.BlockSpec(memory_space=pltpu.VMEM)
    dma = pltpu.SemaphoreType.DMA
    act, gr, gl = pl.pallas_call(
        functools.partial(kernel, z),
        out_shape=(
            jax.ShapeDtypeStruct((z.tok, z.feat), BF),
            jax.ShapeDtypeStruct((z.orow, z.bs) if z.direct else (z.mp, z.pad, z.orow), F32),
            jax.ShapeDtypeStruct((z.orow, z.bs) if z.direct else (z.bs, z.orow), F32),
        ),
        in_specs=[hbm] * 4,
        out_specs=(hbm, vmem, vmem),
        scratch_shapes=[
            pltpu.VMEM((z.mp, z.tok, z.feat), BF),
            pltpu.VMEM((z.tok, z.feat), BF),
            pltpu.VMEM((z.tok, z.feat), BF),
            pltpu.VMEM((z.orow, z.bs), BF),
            pltpu.VMEM((z.orow, z.bs), BF),
            pltpu.VMEM((z.mp, z.pad, z.orow), BF),
            pltpu.VMEM((z.bs, z.orow), BF),
            pltpu.VMEM((z.n, z.pad, z.orow), BF),
            pltpu.VMEM((z.dp, z.bs, z.orow), BF),
            pltpu.VMEM((z.dp, z.orow, z.feat), BF),
            pltpu.VMEM((z.dp, z.orow, z.blocks * z.own), BF),
            pltpu.VMEM((z.groups, z.ng, z.kg), BF),
            pltpu.VMEM((z.jg, z.fj, z.rh), BF),
            pltpu.VMEM((z.groups, z.ng, z.kg), F32),
            pltpu.VMEM((z.jg, z.fj, z.rh), F32),
            pltpu.VMEM((z.n, z.pad, z.orow), BF),
            pltpu.VMEM((z.n, z.pad, z.orow), BF),
            pltpu.VMEM((z.dp, z.bs, z.orow), BF),
            pltpu.VMEM((z.dp, z.bs, z.orow), BF),
            dma((z.mp, CHUNKS)),
            dma((z.mp, CHUNKS)),
            dma((CHUNKS,)),
            dma((CHUNKS,)),
            dma((CHUNKS,)),
            dma((2,)),
            dma, dma, dma, dma, dma, dma, dma, dma,
        ],
        compiler_params=pltpu.CompilerParams(
            collective_id=0, has_side_effects=True, vmem_limit_bytes=60 * 1024 * 1024),
    )(tokens, cotangent, rw, lw)
    if z.direct:
        return act, gr.reshape(z.own, z.rows, z.bs), gl.reshape(z.own, z.rows, z.bs)
    gr = gr[:, :z.own].reshape(z.mp * z.own, z.own, z.rows).transpose(1, 2, 0)
    gl = gl.reshape(z.bs, z.own, z.rows).transpose(1, 2, 0)
    return act, gr, gl


def solution(mesh):
    n_dp, n_mp = mesh.shape["dp"], mesh.shape["mp"]

    def step(tokens, right_weight, left_weight, cotangent):
        z = Sizes(n_dp, n_mp, tokens.shape[0] // n_dp, tokens.shape[1] // n_mp, right_weight.shape[1])
        return jax.shard_map(
            functools.partial(shards, z),
            mesh=mesh,
            in_specs=(P("dp", "mp"), P("mp", "dp", None), P("mp", "dp", None), P("dp", "mp")),
            out_specs=(P("dp", "mp"), P("mp", "dp", None), P("mp", "dp", None)),
            check_vma=False,
        )(tokens, right_weight, left_weight, cotangent)

    return step
```

```python
import functools

import jax
import jax.numpy as jnp
from jax import lax
from jax.experimental import pallas as pl
from jax.experimental.pallas import tpu as pltpu
from jax.sharding import PartitionSpec as P

MESH = pl.DeviceIdType.MESH
BF = jnp.bfloat16
F32 = jnp.float32
CHUNKS = 8


def iota(shape, dim):
    line = tuple(n if axis == dim else 1 for axis, n in enumerate(shape))
    return lax.broadcasted_iota(jnp.int32, line, dim)


def ones_where(cond):
    return jnp.where(cond, 1.0, 0.0).astype(BF)


def dot_nn(a, b):
    return lax.dot_general(a, b, (((1,), (0,)), ((), ())), preferred_element_type=F32)


def dot_nt(a, b):
    return lax.dot_general(a, b, (((1,), (1,)), ((), ())), preferred_element_type=F32)


def dot_tn(a, b):
    return lax.dot_general(a, b, (((0,), (0,)), ((), ())), preferred_element_type=F32)


def join(parts, axis=1):
    return parts[0] if len(parts) == 1 else jnp.concatenate(parts, axis=axis)


class Sizes:
    def __init__(self, n_dp, n_mp, tok_rows, features, width):
        self.dp, self.mp = n_dp, n_mp
        self.tok, self.feat, self.bs = tok_rows, features, width
        self.own = features // width
        self.blocks = self.own * n_mp
        self.rows = width // n_dp
        self.orow = self.own * self.rows
        self.pad = max(self.own, 16)
        self.gs = max(1, 128 // (self.own * self.own))
        self.groups = n_mp // self.gs
        self.ng = self.gs * self.own * self.own
        self.kg = self.gs * features
        self.jg = self.ng // 128
        self.jl = self.own // self.jg
        self.nj = self.ng // self.jg
        self.rh = self.groups * self.nj
        self.fj = self.jl * width
        self.n = n_dp * n_mp
        self.direct = self.pad == self.own and self.orow % 128 == 0
        self.tc = tok_rows // CHUNKS


def kernel(z, x_hbm, cot_hbm, rw_hbm, lw_hbm, act, gr_ref, gl_ref,
           xfull, cot, rw_v, lw_v, rwt, lwt, rg, lg, p1, p2, wt, lt, gracc, glacc,
           rsend, rrecv, lsend, lrecv,
           x_recv, x_send, x_local, c_local, w_local,
           rw_send, rw_recv, lw_send, lw_recv, gr_send, gr_recv, gl_send, gl_recv):
    d, p = lax.axis_index("dp"), lax.axis_index("mp")
    me = d * z.mp + p
    core = lax.rem(p, 2)
    partner = p + 1 - 2 * core
    chip = p // 2
    chips = z.mp // 2

    barrier = pltpu.get_barrier_semaphore()

    @pl.loop(1, z.n)
    def _(s):
        o = lax.rem(me + s, z.n)
        pl.semaphore_signal(barrier, inc=1, device_id=(o // z.mp, lax.rem(o, z.mp)), device_id_type=MESH)

    def rows(c):
        return pl.ds(pl.multiple_of(c * z.tc, z.tc), z.tc)

    def local_x(c):
        return pltpu.make_async_copy(x_hbm.at[rows(c)], xfull.at[p, rows(c)], x_local.at[c])

    def local_c(c):
        return pltpu.make_async_copy(cot_hbm.at[rows(c)], cot.at[rows(c)], c_local.at[c])

    def send_own(c, kind, target):
        return pltpu.make_async_remote_copy(
            src_ref=x_hbm.at[rows(c)], dst_ref=xfull.at[p, rows(c)],
            send_sem=x_send.at[kind, c], recv_sem=x_recv.at[p, c],
            device_id=(d, target), device_id_type=MESH)

    def forward(c, kind, source):
        return pltpu.make_async_remote_copy(
            src_ref=xfull.at[source, rows(c)], dst_ref=xfull.at[source, rows(c)],
            send_sem=x_send.at[kind, c], recv_sem=x_recv.at[source, c],
            device_id=(d, partner), device_id_type=MESH)

    def arrived(c, source):
        pltpu.make_async_remote_copy(
            src_ref=xfull.at[source, rows(c)], dst_ref=xfull.at[source, rows(c)],
            send_sem=x_send.at[0, c], recv_sem=x_recv.at[source, c],
            device_id=(d, partner), device_id_type=MESH).wait_recv()

    def same_core(s):
        return lax.rem(chip + s, chips) * 2 + core

    def other_core(s):
        return lax.rem(chip + s, chips) * 2 + 1 - core

    @pl.loop(0, CHUNKS)
    def _(c):
        local_x(c).start()
        local_c(c).start()

    local_r = pltpu.make_async_copy(rw_hbm, rw_v, w_local.at[0])
    local_r.start()
    local_l = pltpu.make_async_copy(lw_hbm, lw_v, w_local.at[1])
    local_l.start()
    local_r.wait()
    local_l.wait()
    shape = (z.mp * z.pad, z.bs)
    a, b = iota(shape, 0), iota(shape, 1)
    wide = ones_where((a % z.pad < z.own) & (b == (a // z.pad) * z.own + a % z.pad))
    rwt[...] = dot_nt(wide, rw_v[...]).astype(BF).reshape(z.mp, z.pad, z.orow)
    shape = (z.bs, z.bs)
    lwt[...] = dot_nt(ones_where(iota(shape, 0) == iota(shape, 1)), lw_v[...]).astype(BF)
    rg[me] = rwt[p]
    lg[d] = lwt[...]

    pl.semaphore_wait(barrier, z.n - 1)

    def send_x(c):
        for s in range(1, chips):
            send_own(c, s, same_core(s)).start()
        send_own(c, 0, partner).start()

    send_x(0)

    @pl.loop(1, z.n)
    def _(s):
        o = lax.rem(me + s, z.n)
        q = lax.rem(o, z.mp)
        pltpu.make_async_remote_copy(
            src_ref=rwt.at[q], dst_ref=rg.at[me], send_sem=rw_send, recv_sem=rw_recv,
            device_id=(o // z.mp, q), device_id_type=MESH).start()

    @pl.loop(1, z.dp)
    def _(s):
        pltpu.make_async_remote_copy(
            src_ref=lwt, dst_ref=lg.at[d], send_sem=lw_send, recv_sem=lw_recv,
            device_id=(lax.rem(d + s, z.dp), p), device_id_type=MESH).start()

    @pl.loop(1, CHUNKS)
    def _(c):
        send_x(c)

    for dd in range(z.dp):
        shape = (z.orow, z.feat)
        a, b = iota(shape, 0), iota(shape, 1)
        source = (b // z.bs) * z.rows + (b % z.bs) - dd * z.rows
        inside = (b % z.bs) // z.rows == dd
        p1[dd] = ones_where(inside & (a == source))
        shape = (z.orow, z.blocks * z.own)
        a, b = iota(shape, 0), iota(shape, 1)
        jg = b // z.rh
        i_all = (b % z.rh) // z.jl
        j = jg * z.jl + b % z.jl
        inside = i_all // z.rows == dd
        p2[dd] = ones_where(inside & (a == j * z.rows + i_all % z.rows))
    gracc[...] = jnp.zeros_like(gracc)
    glacc[...] = jnp.zeros_like(glacc)

    def count(ref, sem):
        pltpu.make_async_copy(ref, ref, sem).wait()

    count(lg.at[pl.ds(0, z.dp - 1)], lw_recv)
    left = None
    for dd in range(z.dp):
        part = dot_nn(lg[dd], p2[dd])
        left = part if left is None else left + part
    left = left.astype(BF)
    shape = (z.fj, z.bs)
    spread = ones_where(iota(shape, 0) % z.bs == iota(shape, 1))
    for jg in range(z.jg):
        piece = dot_nn(spread, left[:, jg * z.rh:(jg + 1) * z.rh])
        keep = iota((z.fj, z.rh), 0) // z.bs == iota((z.fj, z.rh), 1) % z.jl
        lt[jg] = jnp.where(keep, piece, 0.0).astype(BF)

    count(rg.at[pl.ds(0, z.n - 1)], rw_recv)
    right = None
    for dd in range(z.dp):
        part = dot_nn(rg[dd * z.mp:(dd + 1) * z.mp].reshape(z.mp * z.pad, z.orow), p1[dd])
        right = part if right is None else right + part
    right = right.astype(BF)
    for g in range(z.groups):
        for s in range(z.gs):
            shape = (z.ng, z.mp * z.pad)
            a, b = iota(shape, 0), iota(shape, 1)
            j = (a // z.nj) * z.jl + a % z.jl
            src = (a % z.nj) // (z.own * z.jl)
            pick = ones_where((src == s) & (b == (g * z.gs + s) * z.pad + j))
            piece = dot_nn(pick, right)
            shape = (z.ng, z.feat)
            keep = (iota(shape, 0) // z.jl) % z.own == iota(shape, 1) // z.bs
            wt[g, :, s * z.feat:(s + 1) * z.feat] = jnp.where(keep, piece, 0.0).astype(BF)

    @pl.loop(0, CHUNKS)
    def _(c):
        local_x(c).wait()
        local_c(c).wait()
        for s in range(1, chips):
            arrived(c, same_core(s))
            forward(c, chips + s, same_core(s)).start()
        arrived(c, partner)
        for s in range(1, chips):
            arrived(c, other_core(s))
        r = rows(c)
        xs = [join([xfull[g * z.gs + s, r] for s in range(z.gs)]) for g in range(z.groups)]
        inner = [dot_nt(xs[g], wt[g]).astype(BF) for g in range(z.groups)]
        back = []
        for jg in range(z.jg):
            mixed = join([v[:, jg * z.nj:(jg + 1) * z.nj] for v in inner])
            pre = dot_nt(mixed, lt[jg])
            cdf = 0.5 * (1.0 + lax.erf(pre * 0.7071067811865476))
            slope = cdf + pre * (jnp.exp(-0.5 * pre * pre) * 0.3989422804014327)
            cols = pl.ds(jg * z.fj, z.fj)
            act[r, cols] = (pre * cdf).astype(BF)
            dpre = (cot[r, cols].astype(F32) * slope).astype(BF)
            glacc[jg] += dot_tn(dpre, mixed)
            back.append(dot_nn(dpre, lt[jg]).astype(BF))
        for g in range(z.groups):
            dinner = join([v[:, g * z.nj:(g + 1) * z.nj] for v in back])
            gracc[g] += dot_tn(dinner, xs[g])

    shape = (z.bs, z.fj)
    fold = ones_where(iota(shape, 1) % z.bs == iota(shape, 0))
    lefts = []
    for jg in range(z.jg):
        keep = iota((z.fj, z.rh), 0) // z.bs == iota((z.fj, z.rh), 1) % z.jl
        lefts.append(dot_nn(fold, jnp.where(keep, glacc[jg], 0.0).astype(BF)).astype(BF))
    left = join(lefts)
    for dd in range(z.dp):
        lsend[dd] = dot_nt(left, p2[dd]).astype(BF)

    @pl.loop(1, z.dp)
    def _(s):
        o = lax.rem(d + s, z.dp)
        pltpu.make_async_remote_copy(
            src_ref=lsend.at[o], dst_ref=lrecv.at[d], send_sem=gl_send, recv_sem=gl_recv,
            device_id=(o, p), device_id_type=MESH).start()

    pieces = []
    for g in range(z.groups):
        for s in range(z.gs):
            shape = (z.pad, z.ng)
            a, b = iota(shape, 0), iota(shape, 1)
            j = (b // z.nj) * z.jl + b % z.jl
            src = (b % z.nj) // (z.own * z.jl)
            pick = ones_where((src == s) & (a == j))
            shape = (z.ng, z.feat)
            keep = (iota(shape, 0) // z.jl) % z.own == iota(shape, 1) // z.bs
            piece = jnp.where(keep, gracc[g, :, s * z.feat:(s + 1) * z.feat], 0.0).astype(BF)
            pieces.append(dot_nn(pick, piece).astype(BF))
    pieces = join(pieces, axis=0)
    for dd in range(z.dp):
        owned = dot_nt(pieces, p1[dd]).astype(BF)
        rsend[dd * z.mp:(dd + 1) * z.mp] = owned.reshape(z.mp, z.pad, z.orow)

    @pl.loop(1, z.n)
    def _(s):
        o = lax.rem(me + s, z.n)
        pltpu.make_async_remote_copy(
            src_ref=rsend.at[o], dst_ref=rrecv.at[me], send_sem=gr_send, recv_sem=gr_recv,
            device_id=(o // z.mp, lax.rem(o, z.mp)), device_id_type=MESH).start()

    lrecv[d] = lsend[d]
    rrecv[me] = rsend[me]

    @pl.loop(0, CHUNKS)
    def _(c):
        for s in range(1, chips):
            send_own(c, s, same_core(s)).wait_send()
            forward(c, chips + s, same_core(s)).wait_send()
        send_own(c, 0, partner).wait_send()

    count(rg.at[pl.ds(0, z.n - 1)], rw_send)
    count(lg.at[pl.ds(0, z.dp - 1)], lw_send)

    count(lrecv.at[pl.ds(0, z.dp - 1)], gl_recv)
    total = lrecv[0].astype(F32)
    for dd in range(1, z.dp):
        total = total + lrecv[dd].astype(F32)
    gl_ref[...] = total.T if z.direct else total
    count(rrecv.at[pl.ds(0, z.n - 1)], gr_recv)
    total = rrecv[0:z.mp].astype(F32)
    for dd in range(1, z.dp):
        total = total + rrecv[dd * z.mp:(dd + 1) * z.mp].astype(F32)
    gr_ref[...] = total.reshape(z.blocks, z.orow).T if z.direct else total
    count(lsend.at[pl.ds(0, z.dp - 1)], gl_send)
    count(rsend.at[pl.ds(0, z.n - 1)], gr_send)


def shards(z, tokens, right_weight, left_weight, cotangent):
    rw = right_weight.reshape(z.orow, z.bs)
    lw = left_weight.reshape(z.orow, z.bs)
    hbm = pl.BlockSpec(memory_space=pltpu.HBM)
    vmem = pl.BlockSpec(memory_space=pltpu.VMEM)
    dma = pltpu.SemaphoreType.DMA
    act, gr, gl = pl.pallas_call(
        functools.partial(kernel, z),
        out_shape=(
            pltpu.VMEM((z.tok, z.feat), BF),
            jax.ShapeDtypeStruct((z.orow, z.bs) if z.direct else (z.mp, z.pad, z.orow), F32),
            jax.ShapeDtypeStruct((z.orow, z.bs) if z.direct else (z.bs, z.orow), F32),
        ),
        in_specs=[hbm] * 4,
        out_specs=(vmem, vmem, vmem),
        scratch_shapes=[
            pltpu.VMEM((z.mp, z.tok, z.feat), BF),
            pltpu.VMEM((z.tok, z.feat), BF),
            pltpu.VMEM((z.orow, z.bs), BF),
            pltpu.VMEM((z.orow, z.bs), BF),
            pltpu.VMEM((z.mp, z.pad, z.orow), BF),
            pltpu.VMEM((z.bs, z.orow), BF),
            pltpu.VMEM((z.n, z.pad, z.orow), BF),
            pltpu.VMEM((z.dp, z.bs, z.orow), BF),
            pltpu.VMEM((z.dp, z.orow, z.feat), BF),
            pltpu.VMEM((z.dp, z.orow, z.blocks * z.own), BF),
            pltpu.VMEM((z.groups, z.ng, z.kg), BF),
            pltpu.VMEM((z.jg, z.fj, z.rh), BF),
            pltpu.VMEM((z.groups, z.ng, z.kg), F32),
            pltpu.VMEM((z.jg, z.fj, z.rh), F32),
            pltpu.VMEM((z.n, z.pad, z.orow), BF),
            pltpu.VMEM((z.n, z.pad, z.orow), BF),
            pltpu.VMEM((z.dp, z.bs, z.orow), BF),
            pltpu.VMEM((z.dp, z.bs, z.orow), BF),
            dma((z.mp, CHUNKS)),
            dma((z.mp, CHUNKS)),
            dma((CHUNKS,)),
            dma((CHUNKS,)),
            dma((2,)),
            dma, dma, dma, dma, dma, dma, dma, dma,
        ],
        compiler_params=pltpu.CompilerParams(
            collective_id=0, has_side_effects=True, vmem_limit_bytes=61 * 1024 * 1024),
    )(tokens, cotangent, rw, lw)
    if z.direct:
        return act, gr.reshape(z.own, z.rows, z.bs), gl.reshape(z.own, z.rows, z.bs)
    gr = gr[:, :z.own].reshape(z.mp * z.own, z.own, z.rows).transpose(1, 2, 0)
    gl = gl.reshape(z.bs, z.own, z.rows).transpose(1, 2, 0)
    return act, gr, gl


def solution(mesh):
    n_dp, n_mp = mesh.shape["dp"], mesh.shape["mp"]

    def step(tokens, right_weight, left_weight, cotangent):
        z = Sizes(n_dp, n_mp, tokens.shape[0] // n_dp, tokens.shape[1] // n_mp, right_weight.shape[1])
        return jax.shard_map(
            functools.partial(shards, z),
            mesh=mesh,
            in_specs=(P("dp", "mp"), P("mp", "dp", None), P("mp", "dp", None), P("dp", "mp")),
            out_specs=(P("dp", "mp"), P("mp", "dp", None), P("mp", "dp", None)),
            check_vma=False,
        )(tokens, right_weight, left_weight, cotangent)

    return step
```
